32 devices in a mesh: dp: 4 (over y, x), samp: 4 (over z), col: 2 (over core).
Axes of the slice: x: 2, y: 2, z: 4, core: 2. Of those that a mesh axis runs over, the one named last changes fastest.
Arguments:
- looked_rows: bfloat16 [16, 1920, 128], P(('dp', 'samp'), None, 'col'), may hold values from -6 to 6
- bag_ids: int32 [16, 1920], P(('dp', 'samp')), may hold values from 0 to 959, never falling along the last dimension, each value on 1 to 4 neighbouring positions
- slot_of: int32 [40], replicated, may hold values from 0 to 39, each once
- labels: int32 [384], P(('dp', 'samp')), may hold values 0 or 1
- out_weight: bfloat16 [3, 128], replicated, may hold values from -0.02734375 to 0.02734375
- filter_first: bfloat16 [128, 1521], replicated, may hold values from -0.15625 to 0.15625
- filter_second: bfloat16 [128, 4992], replicated, may hold values from -0.078125 to 0.078125
- filter_third: bfloat16 [128, 4992], replicated, may hold values from -0.078125 to 0.078125
Outputs:
- row_grads: bfloat16 [16, 1920, 128], P(('dp', 'samp'), None, 'col')
- grad_first: float32 [128, 1521], P('dp')
- grad_second: float32 [128, 4992], P('dp')
- grad_third: float32 [128, 4992], P('dp')
The draws below stay inside these ranges and needn't reach their ends.
Inputs may be any that keep to these rules, and one draw needn't show every extreme that they name: `bag_ids`: within each owner's row, bag numbers never fall; each of the 960 bags has 1 to 4 entries and some bag exactly 4. `slot_of`: each slot number once.
All inputs are finite; a program needn't handle non-finite values. No bound on the sum of `labels` on one device may be relied on, other than what follows from the above.
Results may differ from the reference program's by a relative error of at most 0.014.
Values may be sent and summed in bfloat16 or wider, within the bound.
No kernel may reach another device: no remote copies, remote signals or barrier semaphores. Data moves between devices by JAX's collectives and lax.ppermute only.
A program may use at most 64 MiB of HBM per device.

```python
import math
import jax
import jax.numpy as jnp
import numpy as np
from jax import lax

D = 128
FIELDS = 39
H = 128
SLOTS = 40
MOST_BAG = 4
SAMP_DEV = 24
ENTRIES = 1920
TOTAL = 384
N_DP = 4
N_SAMP = 4


def with_ends(array, rng, least, top_value):
    longest = array.shape.index(max(array.shape))
    spots = []
    for shift in (0, 1):
        where = [jax.random.randint(jax.random.fold_in(rng, axis), (), 0, length) for axis, length in enumerate(array.shape)]
        where[longest] = (where[longest] + shift) % array.shape[longest]
        spots.append(tuple(where))
    return array.at[spots[0]].set(least).at[spots[1]].set(top_value)


def level_of(own_key, extent, shards, low, largest):
    def one(dim, blocks):
        draws = jax.random.uniform(jax.random.fold_in(jax.random.fold_in(own_key, 6), dim), (blocks,), jnp.float32, low / len(shards), largest / len(shards))
        return jnp.repeat(jnp.exp(draws), extent[dim] // blocks).reshape((-1,) + (1,) * (len(extent) - dim - 1))

    level = one(*shards[0])
    for cut in shards[1:]:
        level = level * one(*cut)
    return level


def length_profile(count, total, bound, skew):
    loads = [(1 << 20) // math.isqrt(grade ** skew) + 1 for grade in range(2, count + 1)]
    rest, holding = total - bound - (count - 1), [1] * (count - 1)
    while rest > 0:
        movable = [i for i in range(count - 1) if holding[i] < bound]
        mass, left = sum([loads[i] for i in movable]), rest
        for i in movable:
            more = min(bound - holding[i], max(1, left * loads[i] // mass), rest)
            holding[i] = holding[i] + more
            rest = rest - more
    return np.array([bound] + holding)


def uneven_parts(rng, number_of, total, limit, skew):
    if number_of == 2:
        one = jax.random.randint(rng, (), max(1, total - limit), min(limit, total - 1) + 1)
        return jnp.stack([one, total - one])
    tallies = jnp.asarray(length_profile(number_of, total, limit, skew), jnp.int32)
    couples = (number_of - 1) // 2
    source_of, receiver = tallies[1:1 + 2 * couples:2], tallies[2:2 + 2 * couples:2]
    room = jnp.minimum(source_of - 1, limit - receiver)
    passed = jax.random.randint(jax.random.fold_in(rng, 1), (couples,), 0, 1 << 20) % (room + 1)
    tallies = tallies.at[1:1 + 2 * couples:2].set(source_of - passed).at[2:2 + 2 * couples:2].set(receiver + passed)
    return tallies[jax.random.permutation(jax.random.fold_in(rng, 2), number_of)]


def scatter_about(rng, shape, scale, most, split=(), held_as=jnp.bfloat16):
    array = scale * jax.random.normal(rng, shape, jnp.float32)
    if split:
        array = array * level_of(rng, shape, split, -0.22, 0.18)
    return jnp.clip(array, -most, most).astype(held_as)


def setup_inputs(seed: int = 0) -> dict:
    seeds = jax.random.split(jax.random.key(seed), 9)
    return {
        "looked_rows": scatter_about(seeds[0], (N_DP * N_SAMP, ENTRIES, D), 0.8, 6.0, ((0, 16), (2, 2))),
        "bag_ids": jax.vmap(lambda own: jnp.searchsorted(jnp.cumsum(uneven_parts(own, SAMP_DEV * SLOTS, ENTRIES, MOST_BAG, 2)), jnp.arange(ENTRIES), side="right"))(jax.random.split(seeds[1], (N_DP * N_SAMP))).reshape((N_DP * N_SAMP, ENTRIES)).astype(jnp.int32),
        "slot_of": jax.random.permutation(seeds[2], SLOTS).astype(jnp.int32),
        "labels": with_ends((jax.random.randint(seeds[3], (TOTAL,), 0, 3) < 1).astype(jnp.int32), jax.random.fold_in(seeds[3], 1), 0, 1),
        "out_weight": scatter_about(seeds[4], (3, H), (3 * H * D) ** -0.5, 0.02734375),
        "filter_first": scatter_about(seeds[5], (H, FIELDS * FIELDS), (FIELDS * FIELDS) ** -0.5, 0.15625),
        "filter_second": scatter_about(seeds[6], (H, H * FIELDS), (H * FIELDS) ** -0.5, 0.078125),
        "filter_third": scatter_about(seeds[7], (H, H * FIELDS), (H * FIELDS) ** -0.5, 0.078125),
    }


loss_scale = 16.0


def outer_block(previous, anchor):
    rows_here = previous.shape[0]
    spread_rows = previous.astype(jnp.float32)[:, :, None, :] * anchor.astype(jnp.float32)[:, None, :, :]
    rounded = spread_rows.astype(jnp.bfloat16).reshape(rows_here, previous.shape[1] * anchor.shape[1], anchor.shape[2])
    return lax.optimization_barrier(rounded).astype(jnp.float32)


def forward_layer(filter_weight, previous, anchor):
    outer_products = outer_block(previous, anchor)
    projected_maps = jnp.einsum("fn,vnx->vfx", filter_weight.astype(jnp.float32), outer_products, precision=lax.Precision.HIGHEST)
    return projected_maps.astype(jnp.bfloat16)


def backward_layer(filter_weight, cotangent, previous, anchor):
    outer_products = outer_block(previous, anchor)
    broad_cotangent = cotangent.astype(jnp.float32)
    weight_gradient = jnp.einsum("yhn,ymn->hm", broad_cotangent, outer_products, precision=lax.Precision.HIGHEST)
    spread_rows = jnp.einsum("gt,lgi->lti", filter_weight.astype(jnp.float32), broad_cotangent, precision=lax.Precision.HIGHEST)
    spread_rows = spread_rows.reshape(previous.shape[0], previous.shape[1], anchor.shape[1], anchor.shape[2])
    grad_previous = jnp.sum(spread_rows * anchor.astype(jnp.float32)[:, None, :, :], axis=2)
    grad_anchor = jnp.sum(spread_rows * previous.astype(jnp.float32)[:, :, None, :], axis=1)
    return weight_gradient, grad_previous, grad_anchor


def reference(looked_rows, bag_ids, slot_of, labels, out_weight, filter_first, filter_second, filter_third):
    slot_span = SLOTS // N_SAMP
    group_size = SAMP_DEV * N_SAMP
    bag_count = SAMP_DEV * SLOTS
    owners = N_DP * N_SAMP

    def pool_device(operands):
        rows_dev, ids_dev = operands
        member = (ids_dev[None, :] == jnp.arange(bag_count, dtype=jnp.int32)[:, None]).astype(jnp.float32)
        return jnp.dot(member, rows_dev.astype(jnp.float32), precision=lax.Precision.HIGHEST).astype(jnp.bfloat16)

    pooled = lax.map(pool_device, (looked_rows, bag_ids))
    pooled = pooled.reshape(N_DP, N_SAMP, group_size, slot_span, D).transpose(0, 2, 1, 3, 4)
    pooled = pooled.reshape(N_DP * group_size, SLOTS, D)
    field_slots = slot_of[:FIELDS].astype(jnp.int32)
    fields_all = jnp.take(pooled, field_slots, axis=1)
    field_blocks = fields_all.reshape(owners, SAMP_DEV, FIELDS, D)
    label_blocks = labels.reshape(owners, SAMP_DEV).astype(jnp.float32)
    weights_out = out_weight.astype(jnp.float32)

    def per_block(running, operands):
        anchor, targets = operands
        layer_one = forward_layer(filter_first, anchor, anchor)
        layer_two = forward_layer(filter_second, layer_one, anchor)
        layer_three = forward_layer(filter_third, layer_two, anchor)
        maps_one = jnp.sum(layer_one.astype(jnp.float32), axis=2)
        maps_two = jnp.sum(layer_two.astype(jnp.float32), axis=2)
        maps_three = jnp.sum(layer_three.astype(jnp.float32), axis=2)
        logits = jnp.dot(maps_one, weights_out[0], precision=lax.Precision.HIGHEST)
        logits = logits + jnp.dot(maps_two, weights_out[1], precision=lax.Precision.HIGHEST)
        logits = logits + jnp.dot(maps_three, weights_out[2], precision=lax.Precision.HIGHEST)
        residual_slope = loss_scale * (jax.nn.sigmoid(logits) - targets)
        direct_one = (residual_slope[:, None] * weights_out[0][None, :])[:, :, None]
        direct_two = (residual_slope[:, None] * weights_out[1][None, :])[:, :, None]
        direct_three = (residual_slope[:, None] * weights_out[2][None, :])[:, :, None]
        cotan_three = jnp.broadcast_to(direct_three, layer_three.shape).astype(jnp.bfloat16)
        grad_three, back_two, base_three = backward_layer(filter_third, cotan_three, layer_two, anchor)
        cotan_two = (direct_two + back_two).astype(jnp.bfloat16)
        grad_two, back_one, base_two = backward_layer(filter_second, cotan_two, layer_one, anchor)
        cotan_one = (direct_one + back_one).astype(jnp.bfloat16)
        grad_one, back_zero, base_one = backward_layer(filter_first, cotan_one, anchor, anchor)
        grad_fields = (back_zero + base_one + base_two + base_three).astype(jnp.bfloat16)
        return (running[0] + grad_one, running[1] + grad_two, running[2] + grad_three), grad_fields

    starting = (jnp.zeros((H, FIELDS * FIELDS), jnp.float32), jnp.zeros((H, H * FIELDS), jnp.float32), jnp.zeros((H, H * FIELDS), jnp.float32))
    totals, grad_blocks = lax.scan(per_block, starting, (field_blocks, label_blocks))
    grad_fields = grad_blocks.reshape(N_DP * group_size, FIELDS, D)
    slot_grads = jnp.zeros((N_DP * group_size, SLOTS, D), jnp.bfloat16).at[:, field_slots].set(grad_fields)
    bag_grads = slot_grads.reshape(N_DP, group_size, N_SAMP, slot_span, D).transpose(0, 2, 1, 3, 4)
    bag_grads = bag_grads.reshape(owners, bag_count, D)
    row_grads = jnp.take_along_axis(bag_grads, bag_ids.astype(jnp.int32)[:, :, None], axis=1)
    return row_grads, totals[0], totals[1], totals[2]
```

```python
import math

import jax
import jax.numpy as jnp
import numpy as np
from jax import lax
from jax.sharding import PartitionSpec as P


loss_scale = 16.0
f32 = jnp.float32
bf16 = jnp.bfloat16


def pair_table(width):
    half = width // 2
    first = np.tile(np.arange(width), half + 1)
    shift = np.repeat(np.arange(half + 1), width)
    second = (first + shift) % width
    valid = np.ones(first.shape, bool)
    if width % 2 == 0:
        valid = (shift < half) | (first < half)
    return first, second, valid


def symmetric_fold(width):
    first, second, valid = pair_table(width)
    fold = np.zeros((width * width, first.size), np.float32)
    for p in range(first.size):
        if valid[p]:
            fold[first[p] * width + second[p], p] = 1
            fold[second[p] * width + first[p], p] = 1
    return fold


def exchange(x, axis, offset):
    size = lax.axis_size(axis)
    if size & (size - 1) == 0:
        return lax.ppermute(x, axis, [(i, i ^ offset) for i in range(size)])
    return lax.ppermute(x, axis, [(i, (i + offset) % size) for i in range(size)])


def target(axis, offset):
    size = lax.axis_size(axis)
    me = lax.axis_index(axis)
    return me ^ offset if size & (size - 1) == 0 else (me + offset) % size


def origin(axis, offset):
    size = lax.axis_size(axis)
    me = lax.axis_index(axis)
    return me ^ offset if size & (size - 1) == 0 else (me - offset) % size


def scatter_sum(x, axis):
    size = lax.axis_size(axis)
    pick = lambda index: lax.dynamic_index_in_dim(x, index, 0, keepdims=False)
    total = pick(lax.axis_index(axis)).astype(f32)
    for s in range(1, size):
        total = total + exchange(pick(target(axis, s)).astype(bf16), axis, s).astype(f32)
    return total


def spread_sum(x, axis):
    size = lax.axis_size(axis)
    sent = x.astype(bf16)
    total = x.astype(f32)
    for s in range(1, size):
        total = total + exchange(sent, axis, s).astype(f32)
    return total


def collect(x, axis):
    size = lax.axis_size(axis)
    out = jnp.zeros((size,) + x.shape, x.dtype)
    out = lax.dynamic_update_index_in_dim(out, x, lax.axis_index(axis), 0)
    for s in range(1, size):
        out = lax.dynamic_update_index_in_dim(out, exchange(x, axis, s), origin(axis, s), 0)
    return out


def local(
    looked_rows, bag_ids, slot_of, labels, out_weight, filter_first, filter_second, filter_third
):
    samples = labels.shape[0]
    slots = slot_of.shape[0]
    fields = math.isqrt(filter_first.shape[1])
    wide = fields + 1
    maps = filter_first.shape[0]
    bag_count = samples * slots
    owners = lax.axis_size("samp")
    group_size = samples * owners
    slot_span = slots // owners
    entries = bag_ids[0]
    member = (entries[None, :] == jnp.arange(bag_count, dtype=jnp.int32)[:, None]).astype(bf16)
    pooled = jnp.dot(member, looked_rows[0], preferred_element_type=f32).astype(bf16)
    width = pooled.shape[1]
    lanes = samples * width
    pooled = pooled.reshape(group_size, slot_span, width)
    arrived = lax.all_to_all(pooled, "samp", split_axis=0, concat_axis=1, tiled=True)

    fold = jnp.asarray(symmetric_fold(wide), bf16)
    first, second, _ = pair_table(wide)
    pairs = first.size
    weights_out = out_weight.astype(f32)
    mix_third = jnp.dot(out_weight[2], filter_third, preferred_element_type=f32)
    mix = jnp.concatenate(
        [mix_third.reshape(maps, fields).T, weights_out[1][None]], axis=0
    ).astype(bf16)
    inner = jnp.dot(mix, filter_second, preferred_element_type=f32).astype(bf16)
    inner = inner.reshape(wide, maps, fields).transpose(1, 0, 2)
    inner = jnp.pad(inner, ((0, 0), (0, 0), (0, 1)))
    inner = inner.at[:, fields, fields].set(out_weight[0])
    quad = jnp.dot(inner.reshape(maps, wide * wide), fold, preferred_element_type=f32)
    square = jnp.pad(
        filter_first.reshape(maps, fields, fields), ((0, 0), (0, 1), (0, 1))
    ).reshape(maps, wide * wide)
    base = jnp.dot(square, fold, preferred_element_type=f32)
    both = jnp.concatenate([base, quad], axis=0).astype(bf16)
    swapped = jnp.concatenate([quad, base], axis=0).astype(bf16)

    chooser = (slot_of[:fields][:, None] == jnp.arange(slots, dtype=jnp.int32)[None, :]).astype(bf16)
    x0 = jnp.einsum("fk,nkd->fnd", chooser, arrived, preferred_element_type=f32)
    e = jnp.concatenate([x0.reshape(fields, lanes), jnp.ones((1, lanes), f32)], axis=0)
    twice = jnp.concatenate([e, e], axis=0)
    half = wide // 2
    z = jnp.concatenate([(e * twice[k : k + wide]).astype(bf16) for k in range(half + 1)], axis=0)
    xq = jnp.dot(both, z, preferred_element_type=f32)
    logits = jnp.sum((xq[:maps] * xq[maps:]).reshape(maps, samples, width), axis=(0, 2))
    logits = lax.psum(logits, "col")
    slope = loss_scale * (jax.nn.sigmoid(logits) - labels.astype(f32))
    slope_lanes = jnp.broadcast_to(slope[:, None], (samples, width)).reshape(lanes)
    rounded = xq.astype(bf16)
    d = lax.dot_general(swapped, rounded, (((0,), (0,)), ((), ())), preferred_element_type=f32)
    d = d.reshape(half + 1, wide, lanes)
    grad = jnp.zeros((wide, lanes), f32)
    for k in range(half + 1):
        grad = grad + d[k] * twice[k : k + wide]
        back = d[k] * e
        grad = grad + jnp.roll(back, k, axis=0)
    grad_fields = (grad[:fields] * slope_lanes[None]).astype(bf16).reshape(fields, samples, width)
    slot_grads = jnp.einsum(
        "fk,fnd->nkd", chooser, grad_fields, preferred_element_type=f32
    ).astype(bf16)
    returned = lax.all_to_all(slot_grads, "samp", split_axis=1, concat_axis=0, tiled=True)
    row_grads = jnp.einsum(
        "be,bd->ed", member, returned.reshape(bag_count, width), preferred_element_type=f32
    ).astype(bf16)

    scaled = (xq * slope_lanes[None]).astype(bf16)
    stats = lax.dot_general(scaled, z, (((1,), (1,)), ((), ())), preferred_element_type=f32)
    n_dp, n_col = lax.axis_size("dp"), lax.axis_size("col")
    block = maps // (n_dp * n_col)
    stats = stats.reshape(2, n_dp, n_col, block, pairs).transpose(2, 1, 0, 3, 4)
    stats = scatter_sum(stats, "col")
    stats = scatter_sum(stats, "dp")
    stats = spread_sum(stats, "samp").astype(bf16)
    moment_first = stats[1]
    moments = collect(stats[0], "dp")
    moments = collect(moments, "col").transpose(1, 0, 2, 3).reshape(maps, pairs)
    share = collect(moment_first, "col").reshape(maps // n_dp, pairs)
    unfold = jnp.asarray(symmetric_fold(wide).T.reshape(pairs, wide, wide), bf16)
    grad_first = jnp.dot(
        share, unfold[:, :fields, :fields].reshape(pairs, fields * fields), preferred_element_type=f32
    )
    full = jnp.dot(
        moments, unfold[:, :, :fields].reshape(pairs, wide * fields), preferred_element_type=f32
    ).astype(bf16)
    full = full.reshape(maps, wide, fields).transpose(1, 0, 2)
    mine = lax.dynamic_slice_in_dim(mix, lax.axis_index("dp") * (maps // n_dp), maps // n_dp, 1)
    grad_second = lax.dot_general(
        mine, full.reshape(wide, maps * fields), (((0,), (0,)), ((), ())), preferred_element_type=f32
    )
    inner_third = jnp.einsum(
        "am,jm->aj", filter_second, full[:fields].reshape(fields, maps * fields),
        preferred_element_type=f32,
    )
    w_mine = lax.dynamic_slice_in_dim(
        weights_out[2], lax.axis_index("dp") * (maps // n_dp), maps // n_dp, 0
    )
    grad_third = w_mine[:, None] * inner_third.reshape(1, maps * fields)
    return (row_grads[None], grad_first, grad_second, grad_third)


def solution(mesh):
    in_specs = (
        P(("dp", "samp"), None, "col"),
        P(("dp", "samp"), None),
        P(),
        P(("dp", "samp")),
        P(),
        P(),
        P(),
        P(),
    )
    out_specs = (P(("dp", "samp"), None, "col"), P("dp", None), P("dp", None), P("dp", None))
    return jax.shard_map(local, mesh=mesh, in_specs=in_specs, out_specs=out_specs, check_vma=False)
```

```python
import functools
import math

import jax
import jax.numpy as jnp
import numpy as np
from jax import lax
from jax.experimental import pallas as pl
from jax.experimental.pallas import tpu as pltpu
from jax.sharding import PartitionSpec as P


loss_scale = 16.0
f32 = jnp.float32
bf16 = jnp.bfloat16
i32 = jnp.int32
LANES = 128
SUB = 8


def block_offsets(wide):
    starts, at = [], 0
    for j in range(wide):
        starts.append(at)
        at += wide - j // SUB * SUB
    return starts, at


def vmem(n):
    return [pl.BlockSpec(memory_space=pltpu.VMEM)] * n


def kernel_call(body, out_shape, inputs, scratch=(), **kw):
    single = not isinstance(out_shape, (tuple, list))
    return pl.pallas_call(
        body,
        out_shape=out_shape,
        in_specs=vmem(len(inputs)),
        out_specs=vmem(1)[0] if single else tuple(vmem(len(out_shape))),
        scratch_shapes=list(scratch),
        **kw,
    )(*inputs)


def dot(a, b, dims=((1,), (0,))):
    return lax.dot_general(a, b, (dims, ((), ())), preferred_element_type=f32)


def pool_kernel(key_ref, rows_ref, out_ref, *, keys):
    key = key_ref[...]
    rows = rows_ref[...]
    at = lax.broadcasted_iota(i32, (keys, key.shape[1]), 0)
    parts = []
    for s in range(out_ref.shape[1] // rows.shape[1]):
        hot = (at + s * keys == key).astype(f32).astype(bf16)
        parts.append(dot(hot, rows))
    out_ref[...] = jnp.concatenate(parts, axis=1).astype(bf16)


def expand_kernel(key_ref, grads_ref, out_ref, *, keys):
    width = out_ref.shape[1]
    key = key_ref[...]
    at = lax.broadcasted_iota(i32, (key.shape[0], keys), 1)
    half = key // keys
    low = key - half * keys
    hot = (at == low).astype(f32).astype(bf16)
    both = dot(hot, grads_ref[...])
    out = both[:, :width]
    for s in range(1, grads_ref.shape[1] // width):
        out = jnp.where(half == s, both[:, s * width : (s + 1) * width], out)
    out_ref[...] = out.astype(bf16)


def prep_kernel(w1_ref, w2_ref, w3_ref, ow_ref, both_ref, sym_ref, mix_ref, mixt, spread, wt, w1t, fold, *, fields):
    wide = fields + 1
    maps = w1_ref.shape[0]
    starts, pairs = block_offsets(wide)
    lane = lax.broadcasted_iota(i32, (1, LANES), 1)

    def unroll_lanes(get, c):
        tile, off = divmod(c * fields, LANES)
        v = get(tile)
        if off + fields > LANES:
            v = jnp.where(lane >= off, v, get(tile + 1))
        if off:
            v = pltpu.roll(v, LANES - off, 1)
        return jnp.where(lane < fields, v, 0.0)

    third = dot(jnp.broadcast_to(ow_ref[2:3, :], (SUB, maps)), w3_ref[...])
    for c in range(maps):
        v = unroll_lanes(lambda t: third[:, t * LANES : (t + 1) * LANES], c)
        mixt[c : c + 1, :] = v[0:1]
    turned = mixt[...].T
    mix = jnp.concatenate([turned[:fields], ow_ref[1:2, :].astype(f32)], axis=0).astype(bf16)
    mix_ref[...] = mix
    inner = dot(mix, w2_ref[...])
    for c in range(maps):
        spread[c * wide : (c + 1) * wide, :] = unroll_lanes(
            lambda t: inner[:, t * LANES : (t + 1) * LANES], c
        )
    ones = w1_ref.shape[1]
    for t in range(-(-ones // LANES)):
        stop = min(ones, (t + 1) * LANES)
        v = w1_ref[:, t * LANES : stop].astype(f32)
        if stop - t * LANES < LANES:
            v = jnp.concatenate([v, jnp.zeros((maps, LANES - (stop - t * LANES)), f32)], axis=1)
        w1t[t * LANES : (t + 1) * LANES, :] = v.T
    for i in range(wide):
        block = spread[pl.ds(i, maps, stride=wide), :]
        wt[1, i * wide : (i + 1) * wide, :] = block.T[:wide]
        if i < fields:
            wt[0, i * wide : i * wide + fields, :] = w1t[i * fields : (i + 1) * fields, :]
            wt[0, i * wide + fields : (i + 1) * wide, :] = jnp.zeros((1, maps), f32)
        else:
            wt[0, i * wide : (i + 1) * wide, :] = jnp.zeros((wide, maps), f32)
    wt[1, wide * wide - 1 :, :] = ow_ref[0:1, :].astype(f32)
    for part in range(2):
        for j in range(wide):
            low = j // SUB * SUB
            at = starts[j]
            fold[at : at + SUB, part * maps : (part + 1) * maps] = wt[part, j * wide + low : j * wide + low + SUB, :]
            rest = wide - low - SUB
            if rest:
                fold[at + SUB : at + SUB + rest, part * maps : (part + 1) * maps] = (
                    wt[part, j * wide + low + SUB : (j + 1) * wide, :]
                    + wt[part, pl.ds((low + SUB) * wide + j, rest, stride=wide), :]
                )
        for j in range(0, wide, 2):
            rows = [
                wt[part, k * wide : (k + 1) * wide, :] + wt[part, pl.ds(k, wide, stride=wide), :]
                for k in (j, j + 1)
            ]
            sym_ref[j * wide : (j + 2) * wide, (1 - part) * maps : (2 - part) * maps] = jnp.concatenate(
                rows, axis=0
            ).astype(bf16)
    padded = fold.shape[0]
    if padded > pairs:
        fold[pairs:, :] = jnp.zeros((padded - pairs, 2 * maps), f32)
    both_ref[...] = fold[...].T[:, :pairs].astype(bf16)


def forward_kernel(recv_ref, tgt_ref, lab_ref, both_ref, e_ref, xb_ref, slope_ref, stats_ref, z, *, wide, owners, cols):
    starts, pairs = block_offsets(wide)
    span = recv_ref.shape[1]
    arrived = jnp.concatenate(
        [
            jnp.concatenate([recv_ref[j * cols + h] for j in range(owners)], axis=0)
            for h in range(cols)
        ],
        axis=1,
    )
    rows, chunk = e_ref.shape
    hot = (lax.broadcasted_iota(i32, (rows, owners * span), 1) == tgt_ref[...]).astype(f32).astype(bf16)
    e = dot(hot, arrived)
    e_ref[...] = jnp.where(tgt_ref[...] < 0, 1.0, e)
    steps = rows // wide
    for n in range(steps):
        for j in range(0, wide, 2):
            low = j // SUB * SUB
            block = e_ref[n * wide + low : (n + 1) * wide, :]
            both_rows = [block * e_ref[n * wide + k : n * wide + k + 1, :] for k in (j, j + 1)]
            z[starts[j] : starts[j] + 2 * (wide - low), n * chunk : (n + 1) * chunk] = jnp.concatenate(
                both_rows, axis=0
            ).astype(bf16)
    xq = dot(both_ref[...], z[...])
    maps = xq.shape[0] // 2
    xb_ref[...] = xq.astype(bf16)
    product = jnp.sum(xq[:maps] * xq[maps:], axis=0, keepdims=True)
    packs = lab_ref.shape[2]
    lane = lax.broadcasted_iota(i32, (1, LANES), 1)
    for n in range(steps):
        own = product[:, n * chunk : n * chunk + LANES]
        for h in range(1, chunk // LANES):
            own = own + product[:, n * chunk + h * LANES : n * chunk + (h + 1) * LANES]
        slopes = jnp.zeros((1, LANES), f32)
        for s in range(packs):
            mask = lane // (LANES // packs) == s
            logit = jnp.sum(jnp.where(mask, own, 0.0), axis=1, keepdims=True)
            value = loss_scale * (jax.nn.sigmoid(logit) - lab_ref[n, :, s : s + 1])
            slopes = jnp.where(mask, value, slopes)
        for h in range(chunk // LANES):
            slope_ref[:, n * chunk + h * LANES : n * chunk + (h + 1) * LANES] = slopes
    scaled = (xq * slope_ref[...]).astype(bf16)
    stats_ref[...] = dot(scaled, z[...], ((1,), (1,))).astype(bf16)


def backward_kernel(e_ref, xb_ref, slope_ref, sym_ref, tgt_ref, out_ref, grads, *, wide, owners, cols):
    rows, chunk = e_ref.shape
    span = out_ref.shape[1]
    for n in range(rows // wide):
        d = dot(sym_ref[...], xb_ref[:, n * chunk : (n + 1) * chunk])
        total = jnp.zeros((wide, chunk), f32)
        for j in range(wide):
            total = total + d[j * wide : (j + 1) * wide] * e_ref[n * wide + j : n * wide + j + 1, :]
        grads[n * wide : (n + 1) * wide, :] = total * slope_ref[:, n * chunk : (n + 1) * chunk]
    hot = (lax.broadcasted_iota(i32, (owners * span, rows), 0) == tgt_ref[...]).astype(f32).astype(bf16)
    back = dot(hot, grads[...].astype(bf16)).astype(bf16)
    for j in range(owners):
        for h in range(cols):
            out_ref[j * cols + h] = back[j * span : (j + 1) * span, h * LANES : (h + 1) * LANES]


def exchange(x, axis, offset):
    size = lax.axis_size(axis)
    if size & (size - 1) == 0:
        return lax.ppermute(x, axis, [(i, i ^ offset) for i in range(size)])
    return lax.ppermute(x, axis, [(i, (i + offset) % size) for i in range(size)])


def target(axis, offset):
    size = lax.axis_size(axis)
    me = lax.axis_index(axis)
    return me ^ offset if size & (size - 1) == 0 else (me + offset) % size


def origin(axis, offset):
    size = lax.axis_size(axis)
    me = lax.axis_index(axis)
    return me ^ offset if size & (size - 1) == 0 else (me - offset) % size


def scatter_sum(x, axis):
    size = lax.axis_size(axis)
    pick = lambda index: lax.dynamic_index_in_dim(x, index, 0, keepdims=False)
    total = pick(lax.axis_index(axis)).astype(f32)
    for s in range(1, size):
        total = total + exchange(pick(target(axis, s)).astype(bf16), axis, s).astype(f32)
    return total


def spread_sum(x, axis):
    size = lax.axis_size(axis)
    sent = x.astype(bf16)
    total = x.astype(f32)
    for s in range(1, size):
        total = total + exchange(sent, axis, s).astype(f32)
    return total


def collect(x, axis):
    size = lax.axis_size(axis)
    out = jnp.zeros((size,) + x.shape, x.dtype)
    out = lax.dynamic_update_index_in_dim(out, x, lax.axis_index(axis), 0)
    for s in range(1, size):
        out = lax.dynamic_update_index_in_dim(out, exchange(x, axis, s), origin(axis, s), 0)
    return out


def local(
    looked_rows, bag_ids, slot_of, labels, out_weight, filter_first, filter_second, filter_third
):
    slots = slot_of.shape[0]
    fields = math.isqrt(filter_first.shape[1])
    wide = fields + 1
    maps = filter_first.shape[0]
    owners = lax.axis_size("samp")
    n_dp, n_col = lax.axis_size("dp"), lax.axis_size("col")
    peers = owners * n_col
    slot_span = slots // owners
    samples = labels.shape[0] // n_col
    width = looked_rows.shape[2]
    packs = LANES // width
    steps = samples // packs
    used = steps * slot_span
    span = -(-used // 16) * 16
    keys = peers * span
    entries = bag_ids.shape[1]
    starts, pairs = block_offsets(wide)
    chunk = n_col * LANES

    bag = bag_ids
    piece = bag // used
    key = (piece // packs) * span + bag % used + (piece % packs) * keys
    sent = kernel_call(
        functools.partial(pool_kernel, keys=keys),
        jax.ShapeDtypeStruct((keys, LANES), bf16),
        (key, looked_rows[0]),
    )
    group = ("samp", "col")
    arrived = lax.all_to_all(
        sent.reshape(peers, span, LANES), group, split_axis=0, concat_axis=0, tiled=True
    )
    both, sym, mix = kernel_call(
        functools.partial(prep_kernel, fields=fields),
        (
            jax.ShapeDtypeStruct((2 * maps, pairs), bf16),
            jax.ShapeDtypeStruct((wide * wide, 2 * maps), bf16),
            jax.ShapeDtypeStruct((wide, maps), bf16),
        ),
        (filter_first, filter_second, filter_third, out_weight),
        (
            pltpu.VMEM((maps, LANES), f32),
            pltpu.VMEM((maps * wide, LANES), f32),
            pltpu.VMEM((2, wide * wide, maps), f32),
            pltpu.VMEM((-(-filter_first.shape[1] // LANES) * LANES, maps), f32),
            pltpu.VMEM((-(-pairs // LANES) * LANES, 2 * maps), f32),
        ),
    )
    field_slot = slot_of[:fields]
    place = (field_slot // slot_span) * span + field_slot % slot_span
    targets = jnp.arange(steps, dtype=i32)[:, None] * slot_span + place[None, :]
    targets = jnp.pad(targets, ((0, 0), (0, 1)), constant_values=-1).reshape(-1)
    own = lax.dynamic_slice_in_dim(labels, lax.axis_index("col") * samples, samples, 0)
    own = own.reshape(packs, steps).T.astype(f32).reshape(steps, 1, packs)
    rows = steps * wide
    e, xb, slope, stats = kernel_call(
        functools.partial(forward_kernel, wide=wide, owners=owners, cols=n_col),
        (
            jax.ShapeDtypeStruct((rows, chunk), f32),
            jax.ShapeDtypeStruct((2 * maps, steps * chunk), bf16),
            jax.ShapeDtypeStruct((1, steps * chunk), f32),
            jax.ShapeDtypeStruct((2 * maps, pairs), bf16),
        ),
        (arrived, targets[:, None], own, both),
        (pltpu.VMEM((pairs, steps * chunk), bf16),),
    )
    slot_grads = kernel_call(
        functools.partial(backward_kernel, wide=wide, owners=owners, cols=n_col),
        jax.ShapeDtypeStruct((peers, span, LANES), bf16),
        (e, xb, slope, sym, targets[None, :]),
        (pltpu.VMEM((rows, chunk), f32),),
    )
    returned = lax.all_to_all(slot_grads, group, split_axis=0, concat_axis=0, tiled=True)
    row_grads = kernel_call(
        functools.partial(expand_kernel, keys=keys),
        jax.ShapeDtypeStruct((entries, width), bf16),
        (key.reshape(entries, 1), returned.reshape(keys, LANES)),
    )

    block = maps // (n_dp * n_col)
    stats = stats.reshape(2, n_dp, n_col, block, pairs).transpose(2, 1, 0, 3, 4)
    stats = scatter_sum(stats, "col")
    stats = scatter_sum(stats, "dp")
    stats = spread_sum(stats, "samp").astype(bf16)
    moments = collect(stats[0], "dp")
    moments = collect(moments, "col").transpose(1, 0, 2, 3).reshape(maps, pairs)
    share = collect(stats[1], "col").reshape(maps // n_dp, pairs)
    lookup = np.zeros((wide, wide), np.int32)
    for j in range(wide):
        for i in range(wide):
            a, b = min(i, j), max(i, j)
            lookup[j, i] = starts[a] + b - a // SUB * SUB
    grad_first = share[:, lookup[:fields, :fields].reshape(-1)].astype(f32)
    full = moments[:, lookup[:, :fields].reshape(-1)]
    full = full.reshape(maps, wide, fields).transpose(1, 0, 2)
    mine = lax.dynamic_slice_in_dim(mix, lax.axis_index("dp") * (maps // n_dp), maps // n_dp, 1)
    grad_second = dot(mine, full.reshape(wide, maps * fields), ((0,), (0,)))
    inner_third = dot(filter_second, full[:fields].reshape(fields, maps * fields), ((1,), (1,)))
    w_mine = lax.dynamic_slice_in_dim(
        out_weight[2].astype(f32), lax.axis_index("dp") * (maps // n_dp), maps // n_dp, 0
    )
    grad_third = w_mine[:, None] * inner_third.reshape(1, maps * fields)
    return (row_grads[None], grad_first, grad_second, grad_third)


def solution(mesh):
    in_specs = (
        P(("dp", "samp"), None, "col"),
        P(("dp", "samp"), None),
        P(),
        P(("dp", "samp")),
        P(),
        P(),
        P(),
        P(),
    )
    out_specs = (P(("dp", "samp"), None, "col"), P("dp", None), P("dp", None), P("dp", None))
    return jax.shard_map(local, mesh=mesh, in_specs=in_specs, out_specs=out_specs, check_vma=False)
```

```python
import functools
import math

import jax
import jax.numpy as jnp
from jax import lax
from jax.experimental import pallas as pl
from jax.experimental.pallas import tpu as pltpu
from jax.sharding import PartitionSpec as P


loss_scale = 16.0
f32 = jnp.float32
bf16 = jnp.bfloat16
i32 = jnp.int32
LANES = 128
SUB = 8


def block_offsets(wide):
    starts, at = [], 0
    for j in range(wide):
        starts.append(at)
        at += wide - j // SUB * SUB
    return starts, at


def vmem(n):
    return [pl.BlockSpec(memory_space=pltpu.VMEM)] * n


def kernel_call(body, out_shape, inputs, scratch=(), **kw):
    single = not isinstance(out_shape, (tuple, list))
    return pl.pallas_call(
        body,
        out_shape=out_shape,
        in_specs=vmem(len(inputs)),
        out_specs=vmem(1)[0] if single else tuple(vmem(len(out_shape))),
        scratch_shapes=list(scratch),
        **kw,
    )(*inputs)


def dot(a, b, dims=((1,), (0,))):
    return lax.dot_general(a, b, (dims, ((), ())), preferred_element_type=f32)


def bag_rows(bag_ref, used, span, packs):
    bag = bag_ref[...]
    piece = ((bag.astype(f32) + 0.5) * (1.0 / used)).astype(i32)
    dest = ((piece.astype(f32) + 0.5) * (1.0 / packs)).astype(i32)
    return dest * span + bag - piece * used, piece - dest * packs


def pool_kernel(bag_ref, rows_ref, out_ref, *, used, span):
    keys, wide_lanes = out_ref.shape
    packs = wide_lanes // rows_ref.shape[0]
    row, half = bag_rows(bag_ref, used, span, packs)
    at = lax.broadcasted_iota(i32, (keys, row.shape[1]), 0)
    parts = []
    for s in range(packs):
        hot = (at == jnp.where(half == s, row, -1)).astype(f32).astype(bf16)
        parts.append(dot(hot, rows_ref[...], ((1,), (1,))))
    out_ref[...] = jnp.concatenate(parts, axis=1).astype(bf16)


def expand_kernel(bag_ref, grads_ref, out_ref, *, used, span):
    keys, wide_lanes = grads_ref.shape
    width = out_ref.shape[0]
    row, half = bag_rows(bag_ref, used, span, wide_lanes // width)
    at = lax.broadcasted_iota(i32, (keys, row.shape[1]), 0)
    hot = (at == row).astype(f32).astype(bf16)
    both = dot(grads_ref[...], hot, ((0,), (0,)))
    out = both[:width]
    for s in range(1, wide_lanes // width):
        out = jnp.where(half == s, both[s * width : (s + 1) * width], out)
    out_ref[...] = out.astype(bf16)


def segment(get, start, width):
    lane = lax.broadcasted_iota(i32, (1, LANES), 1)
    tile, off = divmod(start, LANES)
    v = get(tile)
    if off + width > LANES:
        v = jnp.where(lane >= off, v, get(tile + 1))
    if off:
        v = pltpu.roll(v, LANES - off, 1)
    return jnp.where(lane < width, v, 0.0)


def place(tiles, v, start, width):
    lane = lax.broadcasted_iota(i32, (1, LANES), 1)
    tile, off = divmod(start, LANES)
    if off:
        v = pltpu.roll(v, off, 1)
    low = jnp.where(lane >= off, v, 0.0) if off + width > LANES else v
    tiles[tile] = tiles[tile] + low if tile in tiles else low
    if off + width > LANES:
        high = jnp.where(lane < off, v, 0.0)
        tiles[tile + 1] = tiles[tile + 1] + high if tile + 1 in tiles else high


def prep_kernel(w1_ref, w2_ref, w3_ref, ow_ref, both_ref, sym_ref, mix_ref, mixt, spread, wt, w1t, fold, *, fields):
    wide = fields + 1
    maps = w1_ref.shape[1]
    starts, pairs = block_offsets(wide)
    third = dot(jnp.broadcast_to(ow_ref[2:3, :], (SUB, maps)), w3_ref[...])
    for c in range(maps):
        v = segment(lambda t: third[:, t * LANES : (t + 1) * LANES], c * fields, fields)
        mixt[c : c + 1, :] = v[0:1]
    turned = mixt[...].T
    ow = ow_ref[...].astype(f32)
    turned = jnp.concatenate(
        [turned[:fields], ow[1:2], ow[2:3], jnp.zeros((LANES - fields - 2, maps), f32)], axis=0
    )
    mix_ref[...] = turned.T
    inner = dot(turned[:wide].astype(bf16), w2_ref[...])
    for c in range(maps):
        spread[c * wide : (c + 1) * wide, :] = segment(
            lambda t: inner[:, t * LANES : (t + 1) * LANES], c * fields, fields
        )
    w1t[...] = w1_ref[...].astype(f32)
    for i in range(wide):
        block = spread[pl.ds(i, maps, stride=wide), :]
        wt[(wide + i) * wide : (wide + i + 1) * wide, :] = block.T[:wide]
        if i < fields:
            wt[i * wide : i * wide + fields, :] = w1t[i * fields : (i + 1) * fields, :]
            wt[i * wide + fields : (i + 1) * wide, :] = jnp.zeros((1, maps), f32)
        else:
            wt[i * wide : (i + 1) * wide, :] = jnp.zeros((wide, maps), f32)
    wt[2 * wide * wide - 1 :, :] = ow_ref[0:1, :].astype(f32)
    for part in range(2):
        top = part * wide * wide
        for j in range(wide):
            low = j // SUB * SUB
            at = starts[j]
            fold[at : at + SUB, part * maps : (part + 1) * maps] = wt[top + j * wide + low : top + j * wide + low + SUB, :]
            rest = wide - low - SUB
            if rest:
                fold[at + SUB : at + SUB + rest, part * maps : (part + 1) * maps] = (
                    wt[top + j * wide + low + SUB : top + (j + 1) * wide, :]
                    + wt[pl.ds(top + (low + SUB) * wide + j, rest, stride=wide), :]
                )
        for j in range(0, wide, 2):
            rows = [
                wt[top + k * wide : top + (k + 1) * wide, :] + wt[pl.ds(top + k, wide, stride=wide), :]
                for k in (j, j + 1)
            ]
            sym_ref[j * wide : (j + 2) * wide, (1 - part) * maps : (2 - part) * maps] = jnp.concatenate(
                rows, axis=0
            ).astype(bf16)
    padded = fold.shape[0]
    if padded > pairs:
        fold[pairs:, :] = jnp.zeros((padded - pairs, 2 * maps), f32)
    both_ref[...] = fold[...].T[:, :pairs].astype(bf16)


def peer_at(axis, offset):
    size = lax.axis_size(axis)
    me = lax.axis_index(axis)
    return me ^ offset if size & (size - 1) == 0 else (me + offset) % size


def forward_kernel(
    recv_ref, slot_ref, label_ref, both_ref, e_ref, xb_ref, slope_ref, hot_ref, *rest, slot_span, owners, n_dp, n_col
):
    sent_refs, z = rest[:n_col], rest[n_col]
    wide = slot_ref.shape[1]
    starts, pairs = block_offsets(wide)
    span = recv_ref.shape[1]
    arrived = jnp.concatenate(
        [
            jnp.concatenate([recv_ref[j * n_col + h] for j in range(owners)], axis=0)
            for h in range(n_col)
        ],
        axis=1,
    )
    rows, chunk = e_ref.shape
    steps = rows // wide
    slot = slot_ref[...].astype(f32)
    owner = ((slot + 0.5) * (1.0 / slot_span)).astype(i32).astype(f32)
    spot = owner * span + slot - owner * slot_span
    spot = jnp.where(lax.broadcasted_iota(i32, (1, wide), 1) < wide - 1, spot, -1e6)
    spot = jnp.concatenate([spot, jnp.zeros((1, LANES - wide), f32)], axis=1)
    column = jnp.broadcast_to(spot, (LANES, LANES)).T[:wide, 0:1]
    lanes = lax.broadcasted_iota(i32, (wide, owners * span), 1).astype(f32)
    hot = jnp.concatenate(
        [(lanes == column + float(n * slot_span)).astype(f32) for n in range(steps)], axis=0
    ).astype(bf16)
    hot_ref[...] = hot
    e = dot(hot, arrived)
    for n in range(steps):
        e_ref[n * wide : (n + 1) * wide, :] = jnp.where(
            lax.broadcasted_iota(i32, (wide, 1), 0) == wide - 1, 1.0, e[n * wide : (n + 1) * wide]
        )
    for n in range(steps):
        for j in range(0, wide, 2):
            low = j // SUB * SUB
            block = e_ref[n * wide + low : (n + 1) * wide, :]
            both_rows = [block * e_ref[n * wide + k : n * wide + k + 1, :] for k in (j, j + 1)]
            z[starts[j] : starts[j] + 2 * (wide - low), n * chunk : (n + 1) * chunk] = jnp.concatenate(
                both_rows, axis=0
            ).astype(bf16)
    xq = dot(both_ref[...], z[...])
    maps = xq.shape[0] // 2
    xb_ref[...] = xq.astype(bf16)
    product = jnp.sum(xq[:maps] * xq[maps:], axis=0, keepdims=True)
    packs = label_ref.shape[1] // (n_col * steps)
    first = lax.axis_index("col") * (packs * steps)
    lane = lax.broadcasted_iota(i32, (1, LANES), 1)
    for n in range(steps):
        own = product[:, n * chunk : n * chunk + LANES]
        for h in range(1, chunk // LANES):
            own = own + product[:, n * chunk + h * LANES : n * chunk + (h + 1) * LANES]
        slopes = jnp.zeros((1, LANES), f32)
        for s in range(packs):
            mask = lane // (LANES // packs) == s
            logit = jnp.sum(jnp.where(mask, own, 0.0), axis=1, keepdims=True)
            label = label_ref[0, first + s * steps + n].astype(f32)
            slopes = jnp.where(mask, loss_scale * (jax.nn.sigmoid(logit) - label), slopes)
        for h in range(chunk // LANES):
            slope_ref[:, n * chunk + h * LANES : n * chunk + (h + 1) * LANES] = slopes
    scaled = (xq * slope_ref[...]).astype(bf16)
    stats = dot(scaled, z[...], ((1,), (1,)))
    block = maps // (n_dp * n_col)
    for s in range(n_col):
        to = peer_at("col", s)
        for d in range(n_dp):
            for part in range(2):
                value = None
                for h in range(n_col):
                    at = part * maps + (d * n_col + h) * block
                    piece = stats[at : at + block]
                    value = piece if value is None else jnp.where(to == h, piece, value)
                sent_refs[s][d, part] = value.astype(bf16)


def backward_kernel(e_ref, xb_ref, slope_ref, sym_ref, hot_ref, out_ref, pick_ref, grads, *, wide, owners, n_col):
    rows, chunk = e_ref.shape
    span = out_ref.shape[1]
    fields = wide - 1
    starts, pairs = block_offsets(wide)
    for n in range(rows // wide):
        d = dot(sym_ref[...], xb_ref[:, n * chunk : (n + 1) * chunk])
        total = jnp.zeros((wide, chunk), f32)
        for j in range(wide):
            total = total + d[j * wide : (j + 1) * wide] * e_ref[n * wide + j : n * wide + j + 1, :]
        grads[n * wide : (n + 1) * wide, :] = total * slope_ref[:, n * chunk : (n + 1) * chunk]
    back = dot(hot_ref[...], grads[...].astype(bf16), ((0,), (0,))).astype(bf16)
    for j in range(owners):
        for h in range(n_col):
            out_ref[j * n_col + h] = back[j * span : (j + 1) * span, h * LANES : (h + 1) * LANES]
    for j in range(0, wide, 2):
        low = j // SUB * SUB
        shape = (wide - low, pick_ref.shape[1])
        i = lax.broadcasted_iota(i32, (wide - low, 1), 0) + low
        column = lax.broadcasted_iota(i32, shape, 1)
        rows_here = []
        for k in (j, j + 1):
            one = jnp.where(i < fields, k * fields + i, -1)
            two = jnp.where(i >= low + SUB, i * fields + k, -1) if k < fields else -1
            rows_here.append(((column == one) | (column == two)).astype(f32))
        pick_ref[starts[j] : starts[j] + 2 * (wide - low), :] = jnp.concatenate(rows_here, axis=0).astype(bf16)


def unfold_kernel(*refs, count, wide):
    parts, (pick_ref, first_ref, flat_ref, spots) = refs[:count], refs[count:]
    fields = wide - 1
    total = parts[0][...].astype(f32)
    for p in parts[1:]:
        total = total + p[...].astype(f32)
    block = total.shape[1]
    total = total.astype(bf16)
    first_ref[...] = dot(total[1], pick_ref[:, : fields * fields]).astype(bf16)
    full = dot(total[0], pick_ref[...])
    tail = -full.shape[1] % LANES
    if tail:
        full = jnp.concatenate([full, jnp.zeros((block, tail), f32)], axis=1)
    for j in range(wide):
        spots[pl.ds(j, block, stride=wide), :] = segment(
            lambda t: full[:, t * LANES : (t + 1) * LANES], j * fields, fields
        )
    tiles = {}
    for c in range(block):
        place(tiles, spots[c * wide : (c + 1) * wide, :], c * fields, fields)
    for t in range(flat_ref.shape[1] // LANES):
        flat_ref[:, t * LANES : (t + 1) * LANES] = tiles[t].astype(bf16)


def final_kernel(flat_ref, first_ref, mix_ref, w2_ref, g1_ref, g2_ref, g3_ref, outer, *, fields):
    wide = fields + 1
    blocks, _, padded = flat_ref.shape
    held = g1_ref.shape[0]
    maps = mix_ref.shape[0]
    seg = maps // blocks * fields
    tiles = {}
    for b in range(blocks):
        for t in range(padded // LANES):
            width = min(LANES, seg - t * LANES)
            place(tiles, flat_ref[b, :, t * LANES : (t + 1) * LANES].astype(f32), b * seg + t * LANES, width)
    flat = jnp.concatenate([tiles[t] for t in range(len(tiles))], axis=1).astype(bf16)
    start = pl.multiple_of(lax.axis_index("dp") * held, held)
    mine = mix_ref[pl.ds(start, held), :]
    g2_ref[...] = dot(mine[:, :wide].astype(bf16), flat)
    outer[...] = dot(w2_ref[...], flat, ((1,), (1,)))
    tiles = {}
    lane = lax.broadcasted_iota(i32, (1, LANES), 1)
    keep = lax.broadcasted_iota(i32, (1, wide), 1) < fields
    for a in range(maps):
        row = jnp.where(keep, outer[a : a + 1, :], 0.0)
        row = jnp.concatenate([row, jnp.zeros((1, LANES - wide), f32)], axis=1)
        place(tiles, jnp.broadcast_to(row, (SUB, LANES)), a * fields, fields)
    weight = jnp.broadcast_to(mine[:, wide : wide + 1], (held, LANES))
    for t in range(len(tiles)):
        g3_ref[:, t * LANES : (t + 1) * LANES] = weight * tiles[t][0:1]
    each = first_ref.shape[1]
    for h in range(first_ref.shape[0]):
        g1_ref[h * each : (h + 1) * each, :] = first_ref[h].astype(f32)


def exchange(x, axis, offset):
    size = lax.axis_size(axis)
    if size & (size - 1) == 0:
        return lax.ppermute(x, axis, [(i, i ^ offset) for i in range(size)])
    return lax.ppermute(x, axis, [(i, (i + offset) % size) for i in range(size)])


def target(axis, offset):
    size = lax.axis_size(axis)
    me = lax.axis_index(axis)
    return me ^ offset if size & (size - 1) == 0 else (me + offset) % size


def origin(axis, offset):
    size = lax.axis_size(axis)
    me = lax.axis_index(axis)
    return me ^ offset if size & (size - 1) == 0 else (me - offset) % size


def scatter_sum(x, axis):
    size = lax.axis_size(axis)
    pick = lambda index: lax.dynamic_index_in_dim(x, index, 0, keepdims=False)
    total = pick(lax.axis_index(axis)).astype(f32)
    for s in range(1, size):
        total = total + exchange(pick(target(axis, s)).astype(bf16), axis, s).astype(f32)
    return total


def gathered(parts, axis):
    out = jnp.zeros((lax.axis_size(axis),) + parts[0].shape, parts[0].dtype)
    for s, part in enumerate(parts):
        out = lax.dynamic_update_index_in_dim(out, part, origin(axis, s) if s else lax.axis_index(axis), 0)
    return out


def local(
    looked_rows, bag_ids, slot_of, labels, out_weight, filter_first, filter_second, filter_third
):
    slots = slot_of.shape[0]
    fields = math.isqrt(filter_first.shape[1])
    wide = fields + 1
    maps = filter_first.shape[0]
    owners = lax.axis_size("samp")
    n_dp, n_col = lax.axis_size("dp"), lax.axis_size("col")
    peers = owners * n_col
    slot_span = slots // owners
    samples = labels.shape[0] // n_col
    width = looked_rows.shape[2]
    packs = LANES // width
    steps = samples // packs
    used = steps * slot_span
    span = -(-used // 16) * 16
    keys = peers * span
    entries = bag_ids.shape[1]
    starts, pairs = block_offsets(wide)
    chunk = n_col * LANES
    rows = steps * wide
    block = maps // (n_dp * n_col)
    held = maps // n_dp
    group = ("samp", "col")

    sent = kernel_call(
        functools.partial(pool_kernel, used=used, span=span),
        jax.ShapeDtypeStruct((keys, LANES), bf16),
        (bag_ids, looked_rows[0].T),
    )
    arrived = lax.all_to_all(
        sent.reshape(peers, span, LANES), group, split_axis=0, concat_axis=0, tiled=True
    )
    both, sym, mix = kernel_call(
        functools.partial(prep_kernel, fields=fields),
        (
            jax.ShapeDtypeStruct((2 * maps, pairs), bf16),
            jax.ShapeDtypeStruct((wide * wide, 2 * maps), bf16),
            jax.ShapeDtypeStruct((maps, LANES), f32),
        ),
        (filter_first.T, filter_second, filter_third, out_weight),
        (
            pltpu.VMEM((maps, LANES), f32),
            pltpu.VMEM((maps * wide, LANES), f32),
            pltpu.VMEM((2 * wide * wide, maps), f32),
            pltpu.VMEM((filter_first.shape[1], maps), f32),
            pltpu.VMEM((-(-pairs // LANES) * LANES, 2 * maps), f32),
        ),
    )
    in_vmem = vmem(1)[0]
    e, xb, slope, hot, *stats = pl.pallas_call(
        functools.partial(
            forward_kernel, slot_span=slot_span, owners=owners, n_dp=n_dp, n_col=n_col
        ),
        out_shape=(
            jax.ShapeDtypeStruct((rows, chunk), f32),
            jax.ShapeDtypeStruct((2 * maps, steps * chunk), bf16),
            jax.ShapeDtypeStruct((1, steps * chunk), f32),
            jax.ShapeDtypeStruct((rows, owners * span), bf16),
        )
        + (jax.ShapeDtypeStruct((n_dp, 2, block, pairs), bf16),) * n_col,
        in_specs=[in_vmem, in_vmem, pl.BlockSpec(memory_space=pltpu.SMEM), in_vmem],
        out_specs=(in_vmem,) * (4 + n_col),
        scratch_shapes=[pltpu.VMEM((pairs, steps * chunk), bf16)],
    )(arrived, slot_of.reshape(1, slots), labels.reshape(1, -1), both)

    total = stats[0].astype(f32)
    for s in range(1, n_col):
        total = total + exchange(stats[s], "col", s).astype(f32)
    summed = scatter_sum(total, "dp").astype(bf16)
    pieces = [summed] + [exchange(summed, "samp", s) for s in range(1, owners)]
    slot_grads, pick = kernel_call(
        functools.partial(backward_kernel, wide=wide, owners=owners, n_col=n_col),
        (
            jax.ShapeDtypeStruct((peers, span, LANES), bf16),
            jax.ShapeDtypeStruct((pairs, wide * fields), bf16),
        ),
        (e, xb, slope, sym, hot),
        (pltpu.VMEM((rows, chunk), f32),),
    )
    packed = -(-block * fields // LANES) * LANES
    first, flat = kernel_call(
        functools.partial(unfold_kernel, count=owners, wide=wide),
        (
            jax.ShapeDtypeStruct((block, fields * fields), bf16),
            jax.ShapeDtypeStruct((wide, packed), bf16),
        ),
        (*pieces, pick),
        (pltpu.VMEM((block * wide, LANES), f32),),
    )
    flat = gathered([flat] + [exchange(flat, "dp", s) for s in range(1, n_dp)], "dp")
    flat = gathered([flat] + [exchange(flat, "col", s) for s in range(1, n_col)], "col")
    first = gathered([first] + [exchange(first, "col", s) for s in range(1, n_col)], "col")
    returned = lax.all_to_all(slot_grads, group, split_axis=0, concat_axis=0, tiled=True)
    row_grads = kernel_call(
        functools.partial(expand_kernel, used=used, span=span),
        jax.ShapeDtypeStruct((width, entries), bf16),
        (bag_ids, returned.reshape(keys, LANES)),
    )
    flat = flat.transpose(1, 0, 2, 3).reshape(n_dp * n_col, wide, packed)
    grad_first, grad_second, grad_third = kernel_call(
        functools.partial(final_kernel, fields=fields),
        (
            jax.ShapeDtypeStruct((held, fields * fields), f32),
            jax.ShapeDtypeStruct((held, maps * fields), f32),
            jax.ShapeDtypeStruct((held, maps * fields), f32),
        ),
        (flat, first, mix, filter_second),
        (pltpu.VMEM((maps, wide), f32),),
    )
    return (row_grads.T[None], grad_first, grad_second, grad_third)


def solution(mesh):
    in_specs = (
        P(("dp", "samp"), None, "col"),
        P(("dp", "samp"), None),
        P(),
        P(("dp", "samp")),
        P(),
        P(),
        P(),
        P(),
    )
    out_specs = (P(("dp", "samp"), None, "col"), P("dp", None), P("dp", None), P("dp", None))
    return jax.shard_map(local, mesh=mesh, in_specs=in_specs, out_specs=out_specs, check_vma=False)
```
